128 devices in a mesh: ba: 16 (over y_lo, z, core), ha: 8 (over y_hi, x).
Axes of the slice: x: 4, y: 4 (y_hi: 2, y_lo: 2; y = y_hi * 2 + y_lo), z: 4, core: 2. Of those that a mesh axis runs over, the one named last changes fastest.
Arguments:
- queries: bfloat16 [4096, 64, 576], P('ba', 'ha'), may hold values from -6 to 6
- out_grad: bfloat16 [4096, 64, 512], P('ba', 'ha'), may hold values from -1.1953125 to 1.1953125
- out_saved: bfloat16 [4096, 64, 512], P('ba', 'ha'), may hold values from -3 to 3
- logsumexp: float32 [4096, 64], P('ba', 'ha'), may hold values from 7 to 9
- parents: int32 [4096], P('ba'), may hold values from 0 to 1023, as said below
- latents: bfloat16 [1024, 576], P(('ba', 'ha')), may hold values from -6 to 6
- hidden: bfloat16 [1024, 7168], P('ba', 'ha'), may hold values from -6 to 6
- latent_weight: bfloat16 [576, 7168], P(None, 'ha'), may hold values from -0.0625 to 0.0625
Outputs:
- query_grad: bfloat16 [4096, 64, 576], P('ba', 'ha')
- weight_grad: bfloat16 [576, 7168], P('ba', 'ha')
- input_grad: bfloat16 [1024, 7168], P('ba', 'ha')
The draws below stay inside these ranges and needn't reach their ends.
Inputs may be any that keep to these rules, and one draw needn't show every extreme that they name: `parents`: the 32 tokens of each aligned block of 32 share one value; some token has 0 and some has 1023.
All inputs are finite; a program needn't handle non-finite values.
Results may differ from the reference program's by a relative error of at most 0.0067.
Values may be sent and summed in bfloat16 or wider, within the bound.
A program may use at most 64 MiB of HBM per device.

```python
import jax
import jax.numpy as jnp
from jax import lax

RANK = 512
ROPE = 64
HEADS = 64
HID = 7168
BRANCH_LEN = 32
TOK_DEV = 256
LAT = 576
TOKENS = 4096
PREFIX = 1024


def draw_parents(key, part):
    first_key, second_key = jax.random.split(jax.random.fold_in(key, 17), 2)
    branch_total = TOKENS // BRANCH_LEN
    device_total = TOKENS // TOK_DEV
    depths = jax.random.randint(first_key, (device_total,), 1, 5)
    picks = jax.random.randint(second_key, (branch_total, 4), 0, PREFIX)
    owner = jnp.arange(branch_total, dtype=jnp.int32) * BRANCH_LEN // TOK_DEV
    chosen = jnp.arange(4, dtype=jnp.int32)[None, :] < depths[owner][:, None]
    forks = jnp.min(jnp.where(chosen, picks, PREFIX), axis=1)
    forks = forks.at[0].set(PREFIX - 1)
    forks = forks.at[branch_total - 1].set(0)
    return jnp.repeat(forks, BRANCH_LEN).astype(jnp.int32)


def steps_of(rng, extent, cuts, low, top_value):
    gain, own = 1.0, jax.random.fold_in(rng, 6)
    for axis_at, parts in cuts:
        heights = jnp.exp(jax.random.uniform(jax.random.fold_in(own, axis_at), (parts,), jnp.float32, low / len(cuts), top_value / len(cuts)))
        gain = gain * jnp.repeat(heights, extent[axis_at] // parts).reshape([-1 if axis == axis_at else 1 for axis in range(len(extent))])
    return gain


def centred(key, dims, spread, reach, cuts=(), kind=jnp.bfloat16):
    array = spread * jax.random.normal(key, dims, jnp.float32)
    if cuts:
        array = array * steps_of(key, dims, cuts, -0.22, 0.18)
    return jnp.clip(array, -reach, reach).astype(kind)


def setup_inputs(seed: int = 0) -> dict:
    seeds = jax.random.split(jax.random.key(seed), 9)
    queries = centred(seeds[0], (TOKENS, HEADS, LAT), 1.0, 6.0, ((0, 16), (1, 8)))
    out_grad = centred(seeds[1], (TOKENS, HEADS, RANK), 0.2, 1.1953125, ((0, 16), (1, 8)))
    out_saved = centred(seeds[2], (TOKENS, HEADS, RANK), 0.5, 3.0, ((0, 16), (1, 8)))
    logsumexp = jnp.clip(7.0 + 2.0 * jax.random.uniform(seeds[3], (TOKENS, HEADS), jnp.float32) ** steps_of(seeds[3], (TOKENS, HEADS), ((0, 16), (1, 8)), -0.2, 0.2), 7.0, 9.0)
    parents = draw_parents(jax.random.fold_in(seeds[8], 71), 0)
    latents = centred(seeds[5], (PREFIX, LAT), 1.0, 6.0, ((0, 128),))
    hidden = centred(seeds[6], (PREFIX, HID), 1.0, 6.0, ((0, 16), (1, 8)))
    latent_weight = centred(seeds[7], (LAT, HID), HID ** -0.5, 0.0625, ((1, 8),))
    return dict(queries=queries, out_grad=out_grad, out_saved=out_saved, logsumexp=logsumexp, parents=parents, latents=latents, hidden=hidden, latent_weight=latent_weight)


softmax_scale = 192.0 ** -0.5


def reference(queries, out_grad, out_saved, logsumexp, parents, latents, hidden, latent_weight):
    key_index = jnp.arange(latents.shape[0], dtype=jnp.int32)
    visible = key_index[None, :] <= parents[:, None]

    def per_head(summed, head_args):
        query_head, grad_head, saved_head, lse_head = head_args
        scores = jnp.dot(query_head, latents.T, preferred_element_type=jnp.float32) * softmax_scale
        weights = jnp.where(visible, jnp.exp(scores - lse_head[:, None]), jnp.float32(0.0))
        grad_prob = jnp.dot(grad_head, latents[:, :RANK].T, preferred_element_type=jnp.float32)
        deltas = jnp.sum(saved_head.astype(jnp.float32) * grad_head.astype(jnp.float32), axis=1)
        grad_score = (weights * (grad_prob - deltas[:, None])).astype(jnp.bfloat16)
        query_head_grad = (softmax_scale * jnp.dot(grad_score, latents, preferred_element_type=jnp.float32)).astype(jnp.bfloat16)
        value_part = jnp.dot(weights.astype(jnp.bfloat16).T, grad_head, preferred_element_type=jnp.float32)
        key_grad = softmax_scale * jnp.dot(grad_score.T, query_head, preferred_element_type=jnp.float32)
        key_grad = key_grad + jnp.pad(value_part, ((0, 0), (0, ROPE)))
        return summed + key_grad, query_head_grad

    head_inputs = (jnp.transpose(queries, (1, 0, 2)), jnp.transpose(out_grad, (1, 0, 2)),
                   jnp.transpose(out_saved, (1, 0, 2)), jnp.transpose(logsumexp, (1, 0)))
    initial = jnp.zeros((latents.shape[0], latents.shape[1]), jnp.float32)
    latent_sum, stacked = lax.scan(per_head, initial, head_inputs)
    query_grad = jnp.transpose(stacked, (1, 0, 2))
    latent_grad = latent_sum.astype(jnp.bfloat16)
    weight_grad = jnp.dot(latent_grad.T, hidden, preferred_element_type=jnp.float32).astype(jnp.bfloat16)
    input_grad = jnp.dot(latent_grad, latent_weight, preferred_element_type=jnp.float32).astype(jnp.bfloat16)
    return (query_grad, weight_grad, input_grad)
```

```python
import jax
import jax.numpy as jnp
from jax import lax
from jax.experimental import pallas as pl
from jax.experimental.pallas import tpu as pltpu
from jax.sharding import PartitionSpec as P

MESH = pl.DeviceIdType.MESH
SCALE = 192.0 ** (-0.5)
RANK = 512
KT = 256
NT = (((1,), (1,)), ((), ()))
NN = (((1,), (0,)), ((), ()))
F32 = jnp.float32
BF = jnp.bfloat16

def attn_kernel(par_ref, q_ref, do_ref, os_ref, lse_ref, k_ref, dq_ref, part_ref, kt_ref, acc_ref, dqt_ref, p_s, ds_s):
    b = pl.program_id(0)
    nb = pl.num_programs(0)
    keys = k_ref.shape[0]
    rows = q_ref.shape[0]

    @pl.when(b == 0)
    def _():
        acc_ref[...] = jnp.zeros_like(acc_ref)
        for i in range(keys // KT):
            kt_ref[:, i * KT:(i + 1) * KT] = k_ref[i * KT:(i + 1) * KT, :].T

    prod = do_ref[...].astype(F32) * os_ref[...].astype(F32)
    part = prod[:, 0:128]
    for i in range(1, RANK // 128):
        part = part + prod[:, i * 128:(i + 1) * 128]
    delta = jnp.sum(part.T, axis=0, keepdims=True) * SCALE
    lse = lse_ref[pl.ds(b, 1), :]
    limit = par_ref[b * (par_ref.shape[0] // nb)]
    count = limit // KT + 1
    dqt_ref[...] = jnp.zeros_like(dqt_ref)

    def tile(i, _):
        at = pl.multiple_of(i * KT, KT)
        kb = k_ref[pl.ds(at, KT), :]
        s = lax.dot_general(kb, q_ref[...], NT, preferred_element_type=F32)
        g = lax.dot_general(kb[:, :RANK], do_ref[...], NT, preferred_element_type=F32)
        idx = at + lax.broadcasted_iota(jnp.int32, (KT, 1), 0)
        p = jnp.where(idx <= limit, jnp.exp(s * SCALE - lse), 0.0)
        ds = (p * (g * SCALE - delta)).astype(BF)
        pb = p.astype(BF)
        acc_ref[pl.ds(at, KT), :] += lax.dot_general(ds, q_ref[...], NN, preferred_element_type=F32)
        acc_ref[pl.ds(at, KT), :RANK] += lax.dot_general(pb, do_ref[...], NN, preferred_element_type=F32)
        dqt_ref[...] += lax.dot_general(kt_ref[:, pl.ds(at, KT)], ds, NN, preferred_element_type=F32)
        return 0

    lax.fori_loop(0, count, tile, 0)
    dq_ref[...] = dqt_ref[...].T.astype(BF)

    @pl.when(b == nb - 1)
    def _():
        part_ref[...] = acc_ref[...].astype(BF)


def attn(parents, q, do, osv, lse, k):
    rows, width = q.shape
    keys = k.shape[0]
    nb = 8
    rb = rows // nb
    return pl.pallas_call(
        attn_kernel,
        grid_spec=pltpu.PrefetchScalarGridSpec(
            num_scalar_prefetch=1,
            grid=(nb,),
            in_specs=[
                pl.BlockSpec((rb, width), lambda b, p: (b, 0)),
                pl.BlockSpec((rb, RANK), lambda b, p: (b, 0)),
                pl.BlockSpec((rb, RANK), lambda b, p: (b, 0)),
                pl.BlockSpec((nb, rb), lambda b, p: (0, 0)),
                pl.BlockSpec((keys, width), lambda b, p: (0, 0)),
            ],
            out_specs=[
                pl.BlockSpec((rb, width), lambda b, p: (b, 0)),
                pl.BlockSpec((keys, width), lambda b, p: (0, 0)),
            ],
            scratch_shapes=[
                pltpu.VMEM((width, keys), BF),
                pltpu.VMEM((keys, width), F32),
                pltpu.VMEM((width, rb), F32),
                pltpu.VMEM((KT, rb), BF),
                pltpu.VMEM((KT, rb), BF),
            ],
        ),
        out_shape=[
            jax.ShapeDtypeStruct((rows, width), BF),
            jax.ShapeDtypeStruct((keys, width), BF),
        ],
        compiler_params=pltpu.CompilerParams(dimension_semantics=("arbitrary",)),
    )(parents, q, do, osv, lse, k)


def place():
    ba, ha = lax.axis_index("ba"), lax.axis_index("ha")
    core = lax.rem(ba, 2)
    z = lax.rem(ba // 2, 4)
    ylo = ba // 8
    x = lax.rem(ha, 4)
    yhi = ha // 4
    return core, x, yhi, ylo, z


def device(core, x, y, z):
    return {"ba": (lax.rem(y, 2) * 4 + z) * 2 + core, "ha": (y // 2) * 4 + x}


def meet(peers):
    barrier = pltpu.get_barrier_semaphore()
    for peer in peers:
        pl.semaphore_signal(barrier, inc=1, device_id=peer, device_id_type=MESH)
    pl.semaphore_wait(barrier, len(peers))


def send(src, dst, send_sem, recv_sem, peer):
    return pltpu.make_async_remote_copy(
        src_ref=src, dst_ref=dst, send_sem=send_sem, recv_sem=recv_sem,
        device_id=peer, device_id_type=MESH,
    )


def gather_kernel(lat_ref, out_ref, plane_s, plane_r, line_s, line_r, pair_s, pair_r):
    core, x, yhi, ylo, z = place()
    y = yhi * 2 + ylo
    first = core == 0
    u, w = jnp.where(first, x, z), jnp.where(first, z, x)

    def at(du, dy, dw):
        pu, pw = lax.rem(u + du, 4), lax.rem(w + dw, 4)
        return device(core, jnp.where(first, pu, pw), lax.rem(y + dy, 4), jnp.where(first, pw, pu))

    partner = device(1 - core, x, y, z)
    plane = [(du, dy) for dy in range(4) for du in range(4) if du or dy]
    plane.sort(key=lambda d: -(min(d[0], 4 - d[0]) + min(d[1], 4 - d[1])))
    meet([at(du, dy, 0) for du, dy in plane] + [at(0, 0, dw) for dw in (1, 2, 3)] + [partner])
    mine = out_ref.at[ylo, z, core, yhi, x]
    copies = []
    for n, (du, dy) in enumerate(plane):
        copy = send(lat_ref, mine, plane_s.at[n], plane_r.at[n], at(du, dy, 0))
        copy.start()
        copies.append(copy)
    out_ref[ylo, z, core, yhi, x] = lat_ref[...]
    for copy in copies:
        copy.wait_recv()

    for c in (0, 1):
        def block(k):
            return out_ref.at[:, k, 0] if c == 0 else out_ref.at[:, :, 1, :, k]

        @pl.when(core == c)
        def _():
            line, pair = [], []
            for n, dw in enumerate((2, 1, 3)):
                copy = send(block(w), block(w), line_s.at[n], line_r.at[n], at(0, 0, dw))
                copy.start()
                line.append(copy)
            own = send(block(w), block(w), pair_s.at[3], pair_r.at[3], partner)
            own.start()
            pair.append(own)
            for n, dw in ((1, 1), (2, 3), (0, 2)):
                line[n].wait_recv()
                src = lax.rem(w + 4 - dw, 4)
                copy = send(block(src), block(src), pair_s.at[n], pair_r.at[n], partner)
                copy.start()
                pair.append(copy)
            for copy in line + pair:
                copy.wait_send()
            for copy in pair:
                copy.wait_recv()

    for copy in copies:
        copy.wait_send()


def gather(latents):
    rows, width = latents.shape
    return pl.pallas_call(
        gather_kernel,
        out_shape=jax.ShapeDtypeStruct((2, 4, 2, 2, 4, rows, width), latents.dtype),
        in_specs=[pl.BlockSpec(memory_space=pltpu.VMEM)],
        out_specs=pl.BlockSpec(memory_space=pltpu.VMEM),
        scratch_shapes=[pltpu.SemaphoreType.DMA((n,)) for n in (15, 15, 3, 3, 4, 4)],
        compiler_params=pltpu.CompilerParams(collective_id=0, has_side_effects=True),
    )(latents)


def total(*blocks):
    out = blocks[0].astype(F32)
    for block in blocks[1:]:
        out = out + block.astype(F32)
    return out


def reduce_kernel(part_ref, hid_ref, rows_ref, cols_ref, hall_ref,
                  got0, acc0, got1, acc1, got2, acc2, colbuf, gotr, gotc,
                  s0, r0, s1, r1, s2, r2, s3, r3, s3c, r3c, s4, r4, s4c, r4c, sh, rh, sp, rp, lsem):
    core, x, yhi, ylo, z = place()
    y = yhi * 2 + ylo
    g, ha = ylo * 4 + z, yhi * 4 + x
    partner = device(1 - core, x, y, z)
    heads = [(dy, dx) for dy in (0, 1) for dx in range(4) if dy or dx]
    heads.sort(key=lambda d: -(2 * d[0] + min(d[1], 4 - d[1])))
    chips = [(dy, dz) for dy in (0, 1) for dz in range(4) if dy or dz]
    chips.sort(key=lambda d: -(d[0] + min(d[1], 4 - d[1])))

    def head_at(dy, dx):
        py, px = lax.rem(yhi + dy, 2), lax.rem(x + dx, 4)
        return py * 4 + px, device(core, px, py * 2 + ylo, z)

    def chip_at(dy, dz):
        py, pz = lax.rem(ylo + dy, 2), lax.rem(z + dz, 4)
        return py * 4 + pz, device(core, x, yhi * 2 + py, pz)

    meet([partner] + [head_at(*d)[1] for d in heads] + [chip_at(*d)[1] for d in chips])

    pending = []
    for c in (0, 1):
        @pl.when(core == c)
        def _():
            send(part_ref.at[:, 1 - c], got0, s0, r0, partner).start()
    first = send(part_ref.at[:, 0], got0, s0, r0, partner)
    own_hidden = pltpu.make_async_copy(hid_ref, hall_ref.at[core, :, g], lsem)
    own_hidden.start()
    hidden = []
    for n, d in enumerate(chips):
        copy = send(hid_ref, hall_ref.at[core, :, g], sh.at[n], rh.at[n], chip_at(*d)[1])
        copy.start()
        hidden.append(copy)
    first.wait_recv()

    for px in range(4):
        for py in range(2):
            acc0[px, py] = total(part_ref[:, core, py, px], got0[:, py, px]).astype(BF)

    line = []
    for n, dx in enumerate((2, 1, 3)):
        to, peer = head_at(0, dx)
        copy = send(acc0.at[to - yhi * 4], got1.at[n], s1.at[n], r1.at[n], peer)
        copy.start()
        line.append(copy)
    for copy in line:
        copy.wait_recv()
    for py in range(2):
        acc1[py] = total(acc0[x, py], got1[0, py], got1[1, py], got1[2, py]).astype(BF)
    other = send(acc1.at[1 - yhi], got2, s2, r2, head_at(1, 0)[1])
    other.start()
    other.wait_recv()
    summed = total(acc1[yhi], got2[...])
    acc2[...] = summed.astype(BF)
    colbuf[...] = jnp.zeros_like(colbuf)
    flat = summed.reshape(64, summed.shape[-1])
    for k in range(8):
        colbuf[k, :, 0:72] = flat[:, k * 72:(k + 1) * 72].astype(BF)
    rows, cols = [], []
    for n, d in enumerate(chips):
        to, peer = chip_at(*d)
        copy = send(acc2.at[to], gotr.at[n], s3.at[n], r3.at[n], peer)
        copy.start()
        rows.append(copy)
        copy = send(colbuf.at[to], gotc.at[n], s3c.at[n], r3c.at[n], peer)
        copy.start()
        cols.append(copy)
    for copy in hidden:
        copy.wait_recv()
    own_hidden.wait()
    swap = send(hall_ref.at[core], hall_ref.at[core], sp.at[0], rp.at[0], partner)
    swap.start()
    for copy in rows + cols:
        copy.wait_recv()
    rows_ref[ha] = total(acc2[g], *[gotr[n] for n in range(7)]).astype(BF)
    cols_ref[core, ha] = total(colbuf[g], *[gotc[n] for n in range(7)]).astype(BF)
    spread = []
    for n, d in enumerate(heads):
        _, peer = head_at(*d)
        copy = send(rows_ref.at[ha], rows_ref.at[ha], s4.at[n], r4.at[n], peer)
        copy.start()
        spread.append(copy)
        copy = send(cols_ref.at[core, ha], cols_ref.at[core, ha], s4c.at[n], r4c.at[n], peer)
        copy.start()
        spread.append(copy)
    for copy in spread:
        copy.wait_recv()
    last = send(cols_ref.at[core], cols_ref.at[core], sp.at[1], rp.at[1], partner)
    last.start()
    first.wait_send()
    for copy in hidden + line + [other] + rows + cols + spread:
        copy.wait_send()
    swap.wait()
    last.wait()


def reduce_and_spread(part, hidden):
    width, columns = part.shape[-1], hidden.shape[-1]
    dma = pltpu.SemaphoreType.DMA
    return pl.pallas_call(
        reduce_kernel,
        out_shape=[
            jax.ShapeDtypeStruct((8, 8, width), BF),
            jax.ShapeDtypeStruct((2, 8, 64, 128), BF),
            jax.ShapeDtypeStruct((2, 8, 8, 8, columns), BF),
        ],
        in_specs=[pl.BlockSpec(memory_space=pltpu.VMEM)] * 2,
        out_specs=[pl.BlockSpec(memory_space=pltpu.VMEM)] * 3,
        scratch_shapes=[
            pltpu.VMEM((8, 2, 4, 8, width), BF),
            pltpu.VMEM((4, 2, 8, 8, width), BF),
            pltpu.VMEM((3, 2, 8, 8, width), BF),
            pltpu.VMEM((2, 8, 8, width), BF),
            pltpu.VMEM((8, 8, width), BF),
            pltpu.VMEM((8, 8, width), BF),
            pltpu.VMEM((8, 64, 128), BF),
            pltpu.VMEM((7, 8, width), BF),
            pltpu.VMEM((7, 64, 128), BF),
            dma, dma, dma((3,)), dma((3,)), dma, dma, dma((7,)), dma((7,)), dma((7,)), dma((7,)),
            dma((7,)), dma((7,)), dma((7,)), dma((7,)), dma((7,)), dma((7,)), dma((2,)), dma((2,)), dma,
        ],
        compiler_params=pltpu.CompilerParams(collective_id=1, has_side_effects=True),
    )(part, hidden)


def on_device(queries, out_grad, out_saved, logsumexp, parents, latents, hidden, latent_weight):
    tokens, heads, width = queries.shape
    rows = tokens * heads
    keys = gather(latents).reshape(-1, width)
    query_grad, part = attn(
        parents, queries.reshape(rows, width), out_grad.reshape(rows, RANK),
        out_saved.reshape(rows, RANK), logsumexp.reshape(8, rows // 8), keys,
    )
    row_block, cols, hidden_all = reduce_and_spread(
        part.reshape(8, 2, 2, 4, 8, width), hidden.reshape(8, 8, -1)
    )
    core = lax.rem(lax.axis_index("ba"), 2)
    cols = lax.dynamic_slice_in_dim(cols.reshape(1024, 128), core * 36, 36, axis=1)
    weight_grad = lax.dot_general(
        cols, hidden_all.reshape(1024, -1), (((0,), (0,)), ((), ())), preferred_element_type=F32
    ).astype(BF)
    input_grad = jnp.dot(
        row_block.reshape(64, width), latent_weight, preferred_element_type=F32
    ).astype(BF)
    return query_grad.reshape(tokens, heads, width), weight_grad, input_grad


def solution(mesh):
    return jax.shard_map(
        on_device,
        mesh=mesh,
        in_specs=(
            P("ba", "ha", None),
            P("ba", "ha", None),
            P("ba", "ha", None),
            P("ba", "ha"),
            P("ba"),
            P(("ba", "ha"), None),
            P("ba", "ha"),
            P(None, "ha"),
        ),
        out_specs=(P("ba", "ha", None), P("ba", "ha"), P("ba", "ha")),
        check_vma=False,
    )
```

```python
import jax
import jax.numpy as jnp
from jax import lax
from jax.experimental import pallas as pl
from jax.experimental.pallas import tpu as pltpu
from jax.sharding import PartitionSpec as P

MESH = pl.DeviceIdType.MESH
SCALE = 192.0 ** (-0.5)
RANK = 512
KT = 256
NT = (((1,), (1,)), ((), ()))
NN = (((1,), (0,)), ((), ()))
F32 = jnp.float32
BF = jnp.bfloat16

def attn_kernel(par_ref, qt_ref, do_ref, ld_ref, k_ref, dq_ref, part_ref, acc_ref, kt_ref, dqt_ref, p0, d0, p1, d1):
    nb = qt_ref.shape[0]
    keys = k_ref.shape[0]
    per = par_ref.shape[0] // nb
    acc_ref[...] = jnp.zeros_like(acc_ref)
    p1[...] = jnp.zeros_like(p1)
    d1[...] = jnp.zeros_like(d1)
    for i in range(keys // KT):
        kt_ref[:, i * KT:(i + 1) * KT] = k_ref[i * KT:(i + 1) * KT, :].T

    def limit_of(b):
        return jnp.where(b < nb, par_ref[jnp.minimum(b, nb - 1) * per], -1)

    def step(b, t, ob, ot, fresh, p_in, d_in, p_out, d_out):
        limit = limit_of(b)
        bb = jnp.minimum(b, nb - 1)
        at = pl.multiple_of(t * KT, KT)
        s = lax.dot_general(k_ref[pl.ds(at, KT), :], qt_ref[bb], NN, preferred_element_type=F32)
        g = lax.dot_general(k_ref[pl.ds(at, KT), :RANK], do_ref[bb], NT, preferred_element_type=F32)
        idx = at + lax.broadcasted_iota(jnp.int32, (KT, 1), 0)
        p = jnp.where(idx <= limit, jnp.exp(s * SCALE - ld_ref[0, pl.ds(bb, 1), :]), 0.0)
        d_out[...] = (p * (g * SCALE - ld_ref[1, pl.ds(bb, 1), :])).astype(BF)
        p_out[...] = p.astype(BF)

        oat = pl.multiple_of(ot * KT, KT)
        ds, pp = d_in[...], p_in[...]
        key = lax.dot_general(ds, qt_ref[ob], NT, preferred_element_type=F32)
        val = lax.dot_general(pp, do_ref[ob], NN, preferred_element_type=F32)
        acc_ref[pl.ds(oat, KT), :RANK] += key[:, :RANK] + val
        acc_ref[pl.ds(oat, KT), RANK:] += key[:, RANK:]
        dq = lax.dot_general(kt_ref[:, pl.ds(oat, KT)], ds, NN, preferred_element_type=F32)
        dqt_ref[ob] = dq + jnp.where(fresh, 0.0, dqt_ref[ob])
        more = (t + 1) * KT <= limit
        nextb = jnp.where(more, b, jnp.minimum(b + 1, nb))
        nextt = jnp.where(more, t + 1, 0)
        return nextb, nextt, bb, t, jnp.logical_and(t == 0, b < nb)

    def trip(_, carry):
        carry = step(*carry, p1, d1, p0, d0)
        return step(*carry, p0, d0, p1, d1)

    steps = 1
    for b in range(nb):
        steps = steps + par_ref[b * per] // KT + 1
    lax.fori_loop(0, (steps + 1) // 2, trip, (0, 0, 0, 0, False))

    for b in range(nb):
        block = dqt_ref[b].astype(BF)
        width = block.shape[1] // nb
        for h in range(nb):
            dq_ref[h, :, b * width:(b + 1) * width] = block[:, h * width:(h + 1) * width]
    part_ref[...] = acc_ref[...].astype(BF)


def core_attn(parents, qt, do, ld, k):
    nb, width, rb = qt.shape
    keys = k.shape[0]
    vm = pl.BlockSpec(memory_space=pltpu.VMEM)
    return pl.pallas_call(
        attn_kernel,
        in_specs=[pl.BlockSpec(memory_space=pltpu.SMEM)] + [vm] * 4,
        out_specs=[vm] * 3,
        scratch_shapes=[
            pltpu.VMEM((width, keys), BF),
            pltpu.VMEM((nb, width, rb), F32),
        ] + [pltpu.VMEM((KT, rb), BF)] * 4,
        out_shape=[
            jax.ShapeDtypeStruct((nb, width, rb), BF),
            jax.ShapeDtypeStruct((keys, width), BF),
            jax.ShapeDtypeStruct((keys, width), F32),
        ],
        compiler_params=pltpu.CompilerParams(vmem_limit_bytes=32 * 2**20),
    )(parents, qt, do, ld, k)

def place():
    ba, ha = lax.axis_index("ba"), lax.axis_index("ha")
    core = lax.rem(ba, 2)
    z = lax.rem(ba // 2, 4)
    ylo = ba // 8
    x = lax.rem(ha, 4)
    yhi = ha // 4
    return core, x, yhi, ylo, z


def device(core, x, y, z):
    return {"ba": (lax.rem(y, 2) * 4 + z) * 2 + core, "ha": (y // 2) * 4 + x}


def meet(peers):
    barrier = pltpu.get_barrier_semaphore()
    for peer in peers:
        pl.semaphore_signal(barrier, inc=1, device_id=peer, device_id_type=MESH)
    pl.semaphore_wait(barrier, len(peers))


def send(src, dst, send_sem, recv_sem, peer):
    return pltpu.make_async_remote_copy(
        src_ref=src, dst_ref=dst, send_sem=send_sem, recv_sem=recv_sem,
        device_id=peer, device_id_type=MESH,
    )


def prepare(b, perm, q_in, do_in, os_in, lse_ref, qt_ref, do_ref, ld_ref):
    heads, tokens = lse_ref.shape
    run = tokens // heads
    lanes = slice(b * run, (b + 1) * run)
    qt_ref[b] = jnp.concatenate([q_in[h, :, lanes] for h in range(heads)], axis=1)
    rows = slice(b * tokens, (b + 1) * tokens)
    grad = lax.dot_general(perm, do_in[rows, :], NN, preferred_element_type=F32)
    saved = lax.dot_general(perm, os_in[rows, :], NN, preferred_element_type=F32)
    do_ref[b] = grad.astype(BF)
    prod = grad * saved
    part = prod[:, 0:128]
    for i in range(1, RANK // 128):
        part = part + prod[:, i * 128:(i + 1) * 128]
    ld_ref[0, b:b + 1, :] = jnp.concatenate([lse_ref[h:h + 1, lanes] for h in range(heads)], axis=1)
    ld_ref[1, b:b + 1, :] = jnp.sum(part.T, axis=0, keepdims=True) * SCALE


def gather_kernel(lat_ref, lse_ref, q_hbm, do_hbm, os_hbm, out_ref, qt_ref, do_ref, ld_ref,
                  q_in, do_in, os_in, plane_s, plane_r, line_s, line_r, pair_s, pair_r, load_s):
    loads = [
        pltpu.make_async_copy(src, dst, load_s.at[n])
        for n, (src, dst) in enumerate(((q_hbm, q_in), (do_hbm, do_in), (os_hbm, os_in)))
    ]
    for load in loads:
        load.start()
    core, x, yhi, ylo, z = place()
    y = yhi * 2 + ylo
    first = core == 0
    u, w = jnp.where(first, x, z), jnp.where(first, z, x)

    def at(du, dy, dw):
        pu, pw = lax.rem(u + du, 4), lax.rem(w + dw, 4)
        return device(core, jnp.where(first, pu, pw), lax.rem(y + dy, 4), jnp.where(first, pw, pu))

    partner = device(1 - core, x, y, z)
    plane = [(du, dy) for dy in range(4) for du in range(4) if du or dy]
    plane.sort(key=lambda d: -(min(d[0], 4 - d[0]) + min(d[1], 4 - d[1])))
    meet([at(du, dy, 0) for du, dy in plane] + [at(0, 0, dw) for dw in (1, 2, 3)] + [partner])
    mine = out_ref.at[ylo, z, core, yhi, x]
    copies = []
    for n, (du, dy) in enumerate(plane):
        copy = send(lat_ref, mine, plane_s.at[n], plane_r.at[n], at(du, dy, 0))
        copy.start()
        copies.append(copy)
    out_ref[ylo, z, core, yhi, x] = lat_ref[...]
    for load in loads:
        load.wait()
    heads, tokens = lse_ref.shape
    row = lax.broadcasted_iota(jnp.int32, (tokens, tokens), 0)
    col = lax.broadcasted_iota(jnp.int32, (tokens, tokens), 1)
    run = tokens // heads
    perm = jnp.where(col == lax.rem(row, run) * heads + row // run, 1.0, 0.0).astype(BF)
    for b in range(heads // 2):
        prepare(b, perm, q_in, do_in, os_in, lse_ref, qt_ref, do_ref, ld_ref)
    for copy in copies:
        copy.wait_recv()

    def block(c, k):
        return out_ref.at[:, k, 0] if c == 0 else out_ref.at[:, :, 1, :, k]

    def line_copy(c, n, dw):
        return send(block(c, w), block(c, w), line_s.at[n], line_r.at[n], at(0, 0, dw))

    def pair_copy(c, n, k):
        return send(block(c, k), block(c, k), pair_s.at[n], pair_r.at[n], partner)

    lines = ((2, 1, 3))
    for c in (0, 1):
        @pl.when(core == c)
        def _():
            for n, dw in enumerate(lines):
                line_copy(c, n, dw).start()
            pair_copy(c, 3, w).start()

    for b in range(heads // 2, heads):
        prepare(b, perm, q_in, do_in, os_in, lse_ref, qt_ref, do_ref, ld_ref)

    for c in (0, 1):
        @pl.when(core == c)
        def _():
            for n, dw in ((1, 1), (2, 3), (0, 2)):
                line_copy(c, n, dw).wait_recv()
                pair_copy(c, n, lax.rem(w + 4 - dw, 4)).start()
            for n, dw in enumerate(lines):
                line_copy(c, n, dw).wait_send()
            for n in range(4):
                pair_copy(c, n, w).wait()

    for copy in copies:
        copy.wait_send()


def gather(latents, lse, q, do, osv):
    rows, width = latents.shape
    heads, _, tokens = q.shape
    vm, hbm = pl.BlockSpec(memory_space=pltpu.VMEM), pl.BlockSpec(memory_space=pltpu.HBM)
    return pl.pallas_call(
        gather_kernel,
        out_shape=[
            jax.ShapeDtypeStruct((2, 4, 2, 2, 4, rows, width), BF),
            jax.ShapeDtypeStruct((heads, width, tokens), BF),
            jax.ShapeDtypeStruct((heads, tokens, RANK), BF),
            jax.ShapeDtypeStruct((2, heads, tokens), F32),
        ],
        in_specs=[vm, vm, hbm, hbm, hbm],
        out_specs=[vm] * 4,
        scratch_shapes=[pltpu.VMEM(a.shape, BF) for a in (q, do, osv)]
        + [pltpu.SemaphoreType.DMA((n,)) for n in (15, 15, 3, 3, 4, 4, 3)],
        compiler_params=pltpu.CompilerParams(
            collective_id=0, has_side_effects=True, vmem_limit_bytes=50 * 2**20
        ),
    )(latents, lse, q, do, osv)


def total(*blocks):
    out = blocks[0].astype(F32)
    for block in blocks[1:]:
        out = out + block.astype(F32)
    return out


def reduce_kernel(part_ref, own_ref, hid_ref, rows_ref, cols_ref, hall_ref,
                  got0, acc0, got1, acc1, keep1, got2, acc2, colbuf, gotr, gotc,
                  s0, r0, s1, r1, s2, r2, s3, r3, s3c, r3c, s4, r4, s4c, r4c, sh, rh, sp, rp, lsem):
    core, x, yhi, ylo, z = place()
    y = yhi * 2 + ylo
    g, ha = ylo * 4 + z, yhi * 4 + x
    partner = device(1 - core, x, y, z)
    heads = [(dy, dx) for dy in (0, 1) for dx in range(4) if dy or dx]
    heads.sort(key=lambda d: -(2 * d[0] + min(d[1], 4 - d[1])))
    chips = [(dy, dz) for dy in (0, 1) for dz in range(4) if dy or dz]
    chips.sort(key=lambda d: -(d[0] + min(d[1], 4 - d[1])))

    def head_at(dy, dx):
        py, px = lax.rem(yhi + dy, 2), lax.rem(x + dx, 4)
        return py * 4 + px, device(core, px, py * 2 + ylo, z)

    def chip_at(dy, dz):
        py, pz = lax.rem(ylo + dy, 2), lax.rem(z + dz, 4)
        return py * 4 + pz, device(core, x, yhi * 2 + py, pz)

    meet([partner] + [head_at(*d)[1] for d in heads] + [chip_at(*d)[1] for d in chips])

    pending = []
    for c in (0, 1):
        @pl.when(core == c)
        def _():
            send(part_ref.at[:, 1 - c], got0, s0, r0, partner).start()
    first = send(part_ref.at[:, 0], got0, s0, r0, partner)
    own_hidden = pltpu.make_async_copy(hid_ref, hall_ref.at[core, :, g], lsem)
    own_hidden.start()
    hidden = []
    for n, d in enumerate(chips):
        copy = send(hid_ref, hall_ref.at[core, :, g], sh.at[n], rh.at[n], chip_at(*d)[1])
        copy.start()
        hidden.append(copy)
    first.wait_recv()

    for px in range(4):
        for py in range(2):
            acc0[px, py] = total(own_ref[:, core, py, px], got0[:, py, px]).astype(BF)

    line = []
    for n, dx in enumerate((2, 1, 3)):
        to, peer = head_at(0, dx)
        copy = send(acc0.at[to - yhi * 4], got1.at[n], s1.at[n], r1.at[n], peer)
        copy.start()
        line.append(copy)
    for copy in line:
        copy.wait_recv()
    for py in range(2):
        summed = total(own_ref[:, core, py, x], got0[:, py, x], got1[0, py], got1[1, py], got1[2, py])
        keep1[py] = summed
        acc1[py] = summed.astype(BF)
    other = send(acc1.at[1 - yhi], got2, s2, r2, head_at(1, 0)[1])
    other.start()
    other.wait_recv()
    summed = total(keep1[yhi], got2[...])
    keep1[0] = summed
    acc2[...] = summed.astype(BF)
    flat = summed.reshape(64, summed.shape[-1])
    colbuf[...] = jnp.zeros_like(colbuf)
    for k in range(8):
        colbuf[k, :, 0:72] = flat[:, k * 72:(k + 1) * 72].astype(BF)
    rows, cols = [], []
    for n, d in enumerate(chips):
        to, peer = chip_at(*d)
        copy = send(acc2.at[to], gotr.at[n], s3.at[n], r3.at[n], peer)
        copy.start()
        rows.append(copy)
        copy = send(colbuf.at[to], gotc.at[n], s3c.at[n], r3c.at[n], peer)
        copy.start()
        cols.append(copy)
    for copy in hidden:
        copy.wait_recv()
    own_hidden.wait()
    swap = send(hall_ref.at[core], hall_ref.at[core], sp.at[0], rp.at[0], partner)
    swap.start()
    for copy in rows + cols:
        copy.wait_recv()
    rows_ref[ha] = total(keep1[0, g], *[gotr[n] for n in range(7)]).astype(BF)
    cols_ref[core, ha] = total(colbuf[g], *[gotc[n] for n in range(7)]).astype(BF)
    spread = []
    for n, d in enumerate(heads):
        _, peer = head_at(*d)
        copy = send(rows_ref.at[ha], rows_ref.at[ha], s4.at[n], r4.at[n], peer)
        copy.start()
        spread.append(copy)
        copy = send(cols_ref.at[core, ha], cols_ref.at[core, ha], s4c.at[n], r4c.at[n], peer)
        copy.start()
        spread.append(copy)
    for copy in spread:
        copy.wait_recv()
    last = send(cols_ref.at[core], cols_ref.at[core], sp.at[1], rp.at[1], partner)
    last.start()
    first.wait_send()
    for copy in hidden + line + [other] + rows + cols + spread:
        copy.wait_send()
    swap.wait()
    last.wait()


def reduce_and_spread(part, own, hidden):
    width, columns = part.shape[-1], hidden.shape[-1]
    dma = pltpu.SemaphoreType.DMA
    return pl.pallas_call(
        reduce_kernel,
        out_shape=[
            jax.ShapeDtypeStruct((8, 8, width), BF),
            jax.ShapeDtypeStruct((2, 8, 64, 128), BF),
            jax.ShapeDtypeStruct((2, 8, 8, 8, columns), BF),
        ],
        in_specs=[pl.BlockSpec(memory_space=pltpu.VMEM)] * 3,
        out_specs=[pl.BlockSpec(memory_space=pltpu.VMEM)] * 3,
        scratch_shapes=[
            pltpu.VMEM((8, 2, 4, 8, width), BF),
            pltpu.VMEM((4, 2, 8, 8, width), BF),
            pltpu.VMEM((3, 2, 8, 8, width), BF),
            pltpu.VMEM((2, 8, 8, width), BF),
            pltpu.VMEM((2, 8, 8, width), F32),
            pltpu.VMEM((8, 8, width), BF),
            pltpu.VMEM((8, 8, width), BF),
            pltpu.VMEM((8, 64, 128), BF),
            pltpu.VMEM((7, 8, width), BF),
            pltpu.VMEM((7, 64, 128), BF),
            dma, dma, dma((3,)), dma((3,)), dma, dma, dma((7,)), dma((7,)), dma((7,)), dma((7,)),
            dma((7,)), dma((7,)), dma((7,)), dma((7,)), dma((7,)), dma((7,)), dma((2,)), dma((2,)), dma,
        ],
        compiler_params=pltpu.CompilerParams(
            collective_id=1, has_side_effects=True, vmem_limit_bytes=20 * 2**20
        ),
    )(part, own, hidden)


def on_device(queries, out_grad, out_saved, logsumexp, parents, latents, hidden, latent_weight):
    tokens, heads, width = queries.shape
    rows = tokens * heads
    keys, qt, do, ld = gather(
        latents, logsumexp.T, queries.transpose(1, 2, 0),
        out_grad.reshape(rows, RANK), out_saved.reshape(rows, RANK),
    )
    query_grad, part, own = core_attn(parents, qt, do, ld, keys.reshape(-1, width))
    shape = (8, 2, 2, 4, 8, width)
    row_block, cols, hidden_all = reduce_and_spread(
        part.reshape(shape), own.reshape(shape), hidden.reshape(8, 8, -1)
    )
    core = lax.rem(lax.axis_index("ba"), 2)
    cols = lax.dynamic_slice_in_dim(cols.reshape(1024, 128), core * 36, 36, axis=1)
    weight_grad = lax.dot_general(
        cols, hidden_all.reshape(1024, -1), (((0,), (0,)), ((), ())), preferred_element_type=F32
    ).astype(BF)
    input_grad = jnp.dot(
        row_block.reshape(64, width), latent_weight, preferred_element_type=F32
    ).astype(BF)
    return query_grad.transpose(2, 0, 1), weight_grad, input_grad


def solution(mesh):
    return jax.shard_map(
        on_device,
        mesh=mesh,
        in_specs=(
            P("ba", "ha", None),
            P("ba", "ha", None),
            P("ba", "ha", None),
            P("ba", "ha"),
            P("ba"),
            P(("ba", "ha"), None),
            P("ba", "ha"),
            P(None, "ha"),
        ),
        out_specs=(P("ba", "ha", None), P("ba", "ha"), P("ba", "ha")),
        check_vma=False,
    )
```

```python
import jax
import jax.numpy as jnp
from jax import lax
from jax.experimental import pallas as pl
from jax.experimental.pallas import tpu as pltpu
from jax.sharding import PartitionSpec as P

MESH = pl.DeviceIdType.MESH
SCALE = 192.0 ** (-0.5)
RANK = 512
KT = 256
NT = (((1,), (1,)), ((), ()))
NN = (((1,), (0,)), ((), ()))
F32 = jnp.float32
BF = jnp.bfloat16

def attn_kernel(par_ref, qt_ref, do_ref, delta_ref, lse_in, k_ref, dq_ref, part_ref, acc_ref, kt_ref, dqt_ref, lse_ref, p0, d0, p1, d1):
    nb = qt_ref.shape[0]
    keys = k_ref.shape[0]
    per = par_ref.shape[0] // nb
    acc_ref[...] = jnp.zeros_like(acc_ref)
    run = lse_in.shape[1] // nb
    for b in range(nb):
        lanes = slice(b * run, (b + 1) * run)
        lse_ref[b:b + 1, :] = jnp.concatenate([lse_in[h:h + 1, lanes] for h in range(nb)], axis=1)
    p1[...] = jnp.zeros_like(p1)
    d1[...] = jnp.zeros_like(d1)
    for i in range(keys // KT):
        kt_ref[:, i * KT:(i + 1) * KT] = k_ref[i * KT:(i + 1) * KT, :].T

    def limit_of(b):
        return jnp.where(b < nb, par_ref[jnp.minimum(b, nb - 1) * per], -1)

    def step(b, t, ob, ot, fresh, p_in, d_in, p_out, d_out):
        limit = limit_of(b)
        bb = jnp.minimum(b, nb - 1)
        at = pl.multiple_of(t * KT, KT)
        s = lax.dot_general(k_ref[pl.ds(at, KT), :], qt_ref[bb], NN, preferred_element_type=F32)
        g = lax.dot_general(k_ref[pl.ds(at, KT), :RANK], do_ref[bb], NT, preferred_element_type=F32)
        idx = at + lax.broadcasted_iota(jnp.int32, (KT, 1), 0)
        p = jnp.where(idx <= limit, jnp.exp(s * SCALE - lse_ref[pl.ds(bb, 1), :]), 0.0)
        d_out[...] = (p * (g - delta_ref[pl.ds(bb, 1), :])).astype(BF)
        p_out[...] = p.astype(BF)

        oat = pl.multiple_of(ot * KT, KT)
        ds, pp = d_in[...], p_in[...]
        key = lax.dot_general(ds, qt_ref[ob], NT, preferred_element_type=F32)
        val = lax.dot_general(pp, do_ref[ob], NN, preferred_element_type=F32)
        acc_ref[pl.ds(oat, KT), :RANK] += key[:, :RANK] * SCALE + val
        acc_ref[pl.ds(oat, KT), RANK:] += key[:, RANK:] * SCALE
        dq = lax.dot_general(kt_ref[:, pl.ds(oat, KT)], ds, NN, preferred_element_type=F32)
        dqt_ref[ob] = dq + jnp.where(fresh, 0.0, dqt_ref[ob])
        more = (t + 1) * KT <= limit
        nextb = jnp.where(more, b, jnp.minimum(b + 1, nb))
        nextt = jnp.where(more, t + 1, 0)
        return nextb, nextt, bb, t, jnp.logical_and(t == 0, b < nb)

    def trip(_, carry):
        carry = step(*carry, p1, d1, p0, d0)
        return step(*carry, p0, d0, p1, d1)

    steps = 1
    for b in range(nb):
        steps = steps + par_ref[b * per] // KT + 1
    lax.fori_loop(0, (steps + 1) // 2, trip, (0, 0, 0, 0, False))

    for b in range(nb):
        block = (dqt_ref[b] * SCALE).astype(BF)
        width = block.shape[1] // nb
        for h in range(nb):
            dq_ref[h, :, b * width:(b + 1) * width] = block[:, h * width:(h + 1) * width]
    part_ref[...] = acc_ref[...].astype(BF)


def core_attn(parents, qt, do, delta, lse, k):
    nb, width, rb = qt.shape
    keys = k.shape[0]
    vm = pl.BlockSpec(memory_space=pltpu.VMEM)
    return pl.pallas_call(
        attn_kernel,
        in_specs=[pl.BlockSpec(memory_space=pltpu.SMEM)] + [vm] * 5,
        out_specs=[vm] * 3,
        scratch_shapes=[
            pltpu.VMEM((width, keys), BF),
            pltpu.VMEM((nb, width, rb), F32),
            pltpu.VMEM((nb, rb), F32),
        ] + [pltpu.VMEM((KT, rb), BF)] * 4,
        out_shape=[
            jax.ShapeDtypeStruct((nb, width, rb), BF),
            jax.ShapeDtypeStruct((keys, width), BF),
            jax.ShapeDtypeStruct((keys, width), F32),
        ],
        compiler_params=pltpu.CompilerParams(vmem_limit_bytes=32 * 2**20),
    )(parents, qt, do, delta, lse, k)

def place():
    ba, ha = lax.axis_index("ba"), lax.axis_index("ha")
    core = lax.rem(ba, 2)
    z = lax.rem(ba // 2, 4)
    ylo = ba // 8
    x = lax.rem(ha, 4)
    yhi = ha // 4
    return core, x, yhi, ylo, z


def device(core, x, y, z):
    return {"ba": (lax.rem(y, 2) * 4 + z) * 2 + core, "ha": (y // 2) * 4 + x}


def meet(peers):
    barrier = pltpu.get_barrier_semaphore()
    for peer in peers:
        pl.semaphore_signal(barrier, inc=1, device_id=peer, device_id_type=MESH)
    pl.semaphore_wait(barrier, len(peers))


def send(src, dst, send_sem, recv_sem, peer):
    return pltpu.make_async_remote_copy(
        src_ref=src, dst_ref=dst, send_sem=send_sem, recv_sem=recv_sem,
        device_id=peer, device_id_type=MESH,
    )


def prepare(b, perm, q_in, do_in, os_in, qt_ref, do_ref, delta_ref):
    heads, _, tokens = q_in.shape
    run = tokens // heads
    lanes = slice(b * run, (b + 1) * run)
    qt_ref[b] = jnp.concatenate([q_in[h, :, lanes] for h in range(heads)], axis=1)
    rows = slice(b * tokens, (b + 1) * tokens)
    grad = lax.dot_general(perm, do_in[rows, :], NN, preferred_element_type=F32)
    saved = lax.dot_general(perm, os_in[rows, :], NN, preferred_element_type=F32)
    do_ref[b] = grad.astype(BF)
    prod = grad * saved
    part = prod[:, 0:128]
    for i in range(1, RANK // 128):
        part = part + prod[:, i * 128:(i + 1) * 128]
    delta_ref[b:b + 1, :] = jnp.sum(part.T, axis=0, keepdims=True)


def gather_kernel(lat_ref, q_hbm, do_hbm, os_hbm, out_ref, qt_ref, do_ref, delta_ref,
                  q_in, do_in, os_in, plane_s, plane_r, line_s, line_r, pair_s, pair_r, load_s):
    loads = [
        pltpu.make_async_copy(src, dst, load_s.at[n])
        for n, (src, dst) in enumerate(((q_hbm, q_in), (do_hbm, do_in), (os_hbm, os_in)))
    ]
    for load in loads:
        load.start()
    core, x, yhi, ylo, z = place()
    y = yhi * 2 + ylo
    first = core == 0
    u, w = jnp.where(first, x, z), jnp.where(first, z, x)

    def at(du, dy, dw):
        pu, pw = lax.rem(u + du, 4), lax.rem(w + dw, 4)
        return device(core, jnp.where(first, pu, pw), lax.rem(y + dy, 4), jnp.where(first, pw, pu))

    partner = device(1 - core, x, y, z)
    plane = [(du, dy) for dy in (2, 1, 3, 0) for du in (2, 1, 3, 0) if du or dy]
    meet([at(du, dy, 0) for du, dy in plane] + [at(0, 0, dw) for dw in (1, 2, 3)] + [partner])
    mine = out_ref.at[ylo, z, core, yhi, x]
    copies = {}
    for n, (du, dy) in enumerate(plane):
        copy = send(lat_ref, mine, plane_s.at[n], plane_r.at[n], at(du, dy, 0))
        copy.start()
        copies[du, dy] = copy
    out_ref[ylo, z, core, yhi, x] = lat_ref[...]
    for load in loads:
        load.wait()
    heads, _, tokens = q_in.shape
    row = lax.broadcasted_iota(jnp.int32, (tokens, tokens), 0)
    col = lax.broadcasted_iota(jnp.int32, (tokens, tokens), 1)
    run = tokens // heads
    perm = jnp.where(col == lax.rem(row, run) * heads + row // run, 1.0, 0.0).astype(BF)

    def ready(lo, hi):
        for b in range(lo, hi):
            prepare(b, perm, q_in, do_in, os_in, qt_ref, do_ref, delta_ref)

    def block(c, k, dy):
        row_y = lax.rem(y + 4 - dy, 4)
        hi, lo = row_y // 2, lax.rem(row_y, 2)
        return out_ref.at[lo, k, 0, hi] if c == 0 else out_ref.at[lo, :, 1, hi, k]

    def line_copy(c, dw, dy, k, hop):
        n = (dw - 1) * 4 + dy
        return send(block(c, k, dy), block(c, k, dy), line_s.at[n], line_r.at[n], at(0, 0, hop))

    def pair_copy(c, dw, dy):
        n, k = dw * 4 + dy, lax.rem(w + 4 - dw, 4)
        return send(block(c, k, dy), block(c, k, dy), pair_s.at[n], pair_r.at[n], partner)

    order, relayed = (0, 1, 3, 2), (0, 1)
    ready(0, 2)
    for dy in order:
        for du in (0, 1, 3, 2):
            if du or dy:
                copies[du, dy].wait_recv()
        for c in (0, 1):
            @pl.when(core == c)
            def _():
                for dw in (1, 3) if dy in relayed else (2, 1, 3):
                    line_copy(c, dw, dy, w, dw).start()
                pair_copy(c, 0, dy).start()
    ready(2, 4)
    for c in (0, 1):
        @pl.when(core == c)
        def _():
            for dy in relayed:
                line_copy(c, 3, dy, w, 3).wait_recv()
                line_copy(c, 2, dy, lax.rem(w + 1, 4), 3).start()
                pair_copy(c, 3, dy).start()
    ready(4, heads)
    for c in (0, 1):
        @pl.when(core == c)
        def _():
            for dy in order:
                for dw in (1, 3):
                    if dw == 3 and dy in relayed:
                        continue
                    line_copy(c, dw, dy, w, dw).wait_recv()
                    pair_copy(c, dw, dy).start()
            for dy in order:
                line_copy(c, 2, dy, w, 2).wait_recv()
                pair_copy(c, 2, dy).start()
            for dy in order:
                for dw in (1, 2, 3):
                    line_copy(c, dw, dy, w, dw).wait_send()
                for dw in range(4):
                    pair_copy(c, dw, dy).wait()

    for copy in copies.values():
        copy.wait_send()


def gather(latents, q, do, osv):
    rows, width = latents.shape
    heads, _, tokens = q.shape
    vm, hbm = pl.BlockSpec(memory_space=pltpu.VMEM), pl.BlockSpec(memory_space=pltpu.HBM)
    return pl.pallas_call(
        gather_kernel,
        out_shape=[
            jax.ShapeDtypeStruct((2, 4, 2, 2, 4, rows, width), BF),
            jax.ShapeDtypeStruct((heads, width, tokens), BF),
            jax.ShapeDtypeStruct((heads, tokens, RANK), BF),
            jax.ShapeDtypeStruct((heads, tokens), F32),
        ],
        in_specs=[vm, hbm, hbm, hbm],
        out_specs=[vm] * 4,
        scratch_shapes=[pltpu.VMEM(a.shape, BF) for a in (q, do, osv)]
        + [pltpu.SemaphoreType.DMA((n,)) for n in (15, 15, 12, 12, 16, 16, 3)],
        compiler_params=pltpu.CompilerParams(
            collective_id=0, has_side_effects=True, vmem_limit_bytes=50 * 2**20
        ),
    )(latents, q, do, osv)


def total(*blocks):
    out = blocks[0].astype(F32)
    for block in blocks[1:]:
        out = out + block.astype(F32)
    return out


def reduce_kernel(part_ref, own_ref, hid_ref, rows_ref, cols_ref, hall_ref,
                  got0, acc0, got1, fwd, acc1, keep1, got2, acc2, colbuf, gotr, gotc,
                  s0, r0, s1, r1, s2, r2, s3, r3, s3c, r3c, s4, r4, s4c, r4c, sh, rh, sp, rp, lsem):
    core, x, yhi, ylo, z = place()
    y = yhi * 2 + ylo
    g, ha = ylo * 4 + z, yhi * 4 + x
    partner = device(1 - core, x, y, z)
    heads = [(dy, dx) for dy in (0, 1) for dx in range(4) if dy or dx]
    heads.sort(key=lambda d: -(2 * d[0] + min(d[1], 4 - d[1])))
    chips = [(dy, dz) for dy in (0, 1) for dz in range(4) if dy or dz]
    chips.sort(key=lambda d: -(d[0] + min(d[1], 4 - d[1])))

    def head_at(dy, dx):
        py, px = lax.rem(yhi + dy, 2), lax.rem(x + dx, 4)
        return py * 4 + px, device(core, px, py * 2 + ylo, z)

    def chip_at(dy, dz):
        py, pz = lax.rem(ylo + dy, 2), lax.rem(z + dz, 4)
        return py * 4 + pz, device(core, x, yhi * 2 + py, pz)

    meet([partner] + [head_at(*d)[1] for d in heads] + [chip_at(*d)[1] for d in chips])

    opp, right, left = lax.rem(x + 2, 4), lax.rem(x + 1, 4), lax.rem(x + 3, 4)
    chunks = (opp, right, left, x)

    def swap_copy(c, n):
        return send(part_ref.at[:, 1 - c, :, chunks[n]], got0.at[n], s0.at[n], r0.at[n], partner)

    for c in (0, 1):
        @pl.when(core == c)
        def _():
            for n in range(4):
                swap_copy(c, n).start()
    own_hidden = pltpu.make_async_copy(hid_ref, hall_ref.at[core, :, g], lsem)
    own_hidden.start()
    hidden = []
    for n, d in enumerate(chips):
        copy = send(hid_ref, hall_ref.at[core, :, g], sh.at[n], rh.at[n], chip_at(*d)[1])
        copy.start()
        hidden.append(copy)
    def paired(n, py):
        return total(own_ref[:, core, py, chunks[n]], got0[n, :, py])

    def line_copy(n, src, dst, dx):
        return send(src, dst, s1.at[n], r1.at[n], head_at(0, dx)[1])

    line = [
        line_copy(0, acc0.at[1, 0], got1.at[0, 0], 1),
        line_copy(1, acc0.at[1, 1], got1.at[0, 1], 1),
        line_copy(2, acc0.at[2, 0], got1.at[1, 0], 3),
        line_copy(3, acc0.at[2, 1], got1.at[1, 1], 3),
        line_copy(4, acc0.at[0, 0], fwd.at[0], 1),
        line_copy(5, acc0.at[0, 1], fwd.at[1], 3),
    ]
    swap_copy(0, 0).wait_recv()
    acc0[0, 0] = paired(0, 0).astype(BF)
    line[4].start()
    acc0[0, 1] = paired(0, 1).astype(BF)
    line[5].start()
    swap_copy(0, 1).wait_recv()
    acc0[1, 1] = paired(1, 1).astype(BF)
    line[1].start()
    swap_copy(0, 2).wait_recv()
    acc0[2, 0] = paired(2, 0).astype(BF)
    line[2].start()
    swap_copy(0, 3).wait_recv()
    for py in range(2):
        keep1[py] = paired(3, py)
    line[4].wait_recv()
    acc0[1, 0] = (paired(1, 0) + fwd[0].astype(F32)).astype(BF)
    line[0].start()
    line[5].wait_recv()
    acc0[2, 1] = (paired(2, 1) + fwd[1].astype(F32)).astype(BF)
    line[3].start()
    for n in range(4):
        line[n].wait_recv()
    acc1[...] = total(keep1[1 - yhi], got1[0, 1 - yhi], got1[1, 1 - yhi]).astype(BF)
    other = send(acc1, got2, s2, r2, head_at(1, 0)[1])
    other.start()
    keep1[yhi] = total(keep1[yhi], got1[0, yhi], got1[1, yhi])
    other.wait_recv()
    summed = total(keep1[yhi], got2[...])
    keep1[0] = summed
    acc2[...] = summed.astype(BF)
    flat = summed.reshape(64, summed.shape[-1])
    colbuf[...] = jnp.zeros_like(colbuf)
    for k in range(8):
        colbuf[k, :, 0:72] = flat[:, k * 72:(k + 1) * 72].astype(BF)
    rows, cols = [], []
    for n, d in enumerate(chips):
        to, peer = chip_at(*d)
        copy = send(acc2.at[to], gotr.at[n], s3.at[n], r3.at[n], peer)
        copy.start()
        rows.append(copy)
        copy = send(colbuf.at[to], gotc.at[n], s3c.at[n], r3c.at[n], peer)
        copy.start()
        cols.append(copy)
    for copy in hidden:
        copy.wait_recv()
    own_hidden.wait()
    swap = send(hall_ref.at[core], hall_ref.at[core], sp.at[0], rp.at[0], partner)
    swap.start()
    for copy in rows + cols:
        copy.wait_recv()
    rows_ref[ha] = total(keep1[0, g], *[gotr[n] for n in range(7)]).astype(BF)
    cols_ref[core, ha] = total(colbuf[g], *[gotc[n] for n in range(7)]).astype(BF)
    spread = []
    for n, d in enumerate(heads):
        _, peer = head_at(*d)
        copy = send(rows_ref.at[ha], rows_ref.at[ha], s4.at[n], r4.at[n], peer)
        copy.start()
        spread.append(copy)
        copy = send(cols_ref.at[core, ha], cols_ref.at[core, ha], s4c.at[n], r4c.at[n], peer)
        copy.start()
        spread.append(copy)
    for copy in spread:
        copy.wait_recv()
    last = send(cols_ref.at[core], cols_ref.at[core], sp.at[1], rp.at[1], partner)
    last.start()
    for n in range(4):
        swap_copy(0, n).wait_send()
    for copy in hidden + line + [other] + rows + cols + spread:
        copy.wait_send()
    swap.wait()
    last.wait()


def reduce_and_spread(part, own, hidden):
    width, columns = part.shape[-1], hidden.shape[-1]
    dma = pltpu.SemaphoreType.DMA
    return pl.pallas_call(
        reduce_kernel,
        out_shape=[
            jax.ShapeDtypeStruct((8, 8, width), BF),
            jax.ShapeDtypeStruct((2, 8, 64, 128), BF),
            jax.ShapeDtypeStruct((2, 8, 8, 8, columns), BF),
        ],
        in_specs=[pl.BlockSpec(memory_space=pltpu.VMEM)] * 3,
        out_specs=[pl.BlockSpec(memory_space=pltpu.VMEM)] * 3,
        scratch_shapes=[
            pltpu.VMEM((4, 8, 2, 8, width), BF),
            pltpu.VMEM((3, 2, 8, 8, width), BF),
            pltpu.VMEM((2, 2, 8, 8, width), BF),
            pltpu.VMEM((2, 8, 8, width), BF),
            pltpu.VMEM((8, 8, width), BF),
            pltpu.VMEM((2, 8, 8, width), F32),
            pltpu.VMEM((8, 8, width), BF),
            pltpu.VMEM((8, 8, width), BF),
            pltpu.VMEM((8, 64, 128), BF),
            pltpu.VMEM((7, 8, width), BF),
            pltpu.VMEM((7, 64, 128), BF),
            dma((4,)), dma((4,)), dma((6,)), dma((6,)), dma, dma, dma((7,)), dma((7,)), dma((7,)), dma((7,)),
            dma((7,)), dma((7,)), dma((7,)), dma((7,)), dma((7,)), dma((7,)), dma((2,)), dma((2,)), dma,
        ],
        compiler_params=pltpu.CompilerParams(
            collective_id=1, has_side_effects=True, vmem_limit_bytes=20 * 2**20
        ),
    )(part, own, hidden)


def on_device(queries, out_grad, out_saved, logsumexp, parents, latents, hidden, latent_weight):
    tokens, heads, width = queries.shape
    rows = tokens * heads
    keys, qt, do, delta = gather(
        latents, queries.transpose(1, 2, 0),
        out_grad.reshape(rows, RANK), out_saved.reshape(rows, RANK),
    )
    query_grad, part, own = core_attn(
        parents, qt, do, delta, logsumexp.T, keys.reshape(-1, width)
    )
    shape = (8, 2, 2, 4, 8, width)
    row_block, cols, hidden_all = reduce_and_spread(
        part.reshape(shape), own.reshape(shape), hidden.reshape(8, 8, -1)
    )
    core = lax.rem(lax.axis_index("ba"), 2)
    cols = lax.dynamic_slice_in_dim(cols.reshape(1024, 128), core * 36, 36, axis=1)
    weight_grad = lax.dot_general(
        cols, hidden_all.reshape(1024, -1), (((0,), (0,)), ((), ())), preferred_element_type=F32
    ).astype(BF)
    input_grad = jnp.dot(
        row_block.reshape(64, width), latent_weight, preferred_element_type=F32
    ).astype(BF)
    return query_grad.transpose(2, 0, 1), weight_grad, input_grad


def solution(mesh):
    return jax.shard_map(
        on_device,
        mesh=mesh,
        in_specs=(
            P("ba", "ha", None),
            P("ba", "ha", None),
            P("ba", "ha", None),
            P("ba", "ha"),
            P("ba"),
            P(("ba", "ha"), None),
            P("ba", "ha"),
            P(None, "ha"),
        ),
        out_specs=(P("ba", "ha", None), P("ba", "ha"), P("ba", "ha")),
        check_vma=False,
    )
```

```python
import jax
import jax.numpy as jnp
from jax import lax
from jax.experimental import pallas as pl
from jax.experimental.pallas import tpu as pltpu
from jax.sharding import PartitionSpec as P

MESH = pl.DeviceIdType.MESH
SCALE = 192.0 ** (-0.5)
RANK = 512
KT = 256
NT = (((1,), (1,)), ((), ()))
NN = (((1,), (0,)), ((), ()))
F32 = jnp.float32
BF = jnp.bfloat16

def attn_kernel(par_ref, qt_hbm, do_ref, delta_ref, lse_in, k_ref, dq_hbm, part_ref, own_ref, acc_ref, kt_ref, dqt_ref, lse_ref, qt_ref, dq_ref, p0, d0, p1, d1, load_s, out_s):
    nb = qt_ref.shape[0]
    for b in range(nb):
        pltpu.make_async_copy(qt_hbm.at[b], qt_ref.at[b], load_s.at[b]).start()
    keys = k_ref.shape[0]
    per = par_ref.shape[0] // nb
    acc_ref[...] = jnp.zeros_like(acc_ref)
    run = lse_in.shape[1] // nb
    for b in range(nb):
        lanes = slice(b * run, (b + 1) * run)
        lse_ref[b:b + 1, :] = jnp.concatenate([lse_in[h:h + 1, lanes] for h in range(nb)], axis=1)
    p1[...] = jnp.zeros_like(p1)
    d1[...] = jnp.zeros_like(d1)
    for i in range(keys // KT):
        kt_ref[:, i * KT:(i + 1) * KT] = k_ref[i * KT:(i + 1) * KT, :].T

    def limit_of(b):
        return jnp.where(b < nb, par_ref[jnp.minimum(b, nb - 1) * per], -1)

    def step(b, t, ob, ot, fresh, p_in, d_in, p_out, d_out):
        limit = limit_of(b)
        bb = jnp.minimum(b, nb - 1)
        at = pl.multiple_of(t * KT, KT)
        s = lax.dot_general(k_ref[pl.ds(at, KT), :], qt_ref[bb], NN, preferred_element_type=F32)
        g = lax.dot_general(k_ref[pl.ds(at, KT), :RANK], do_ref[bb], NT, preferred_element_type=F32)
        idx = at + lax.broadcasted_iota(jnp.int32, (KT, 1), 0)
        p = jnp.where(idx <= limit, jnp.exp(s * SCALE - lse_ref[pl.ds(bb, 1), :]), 0.0)
        d_out[...] = (p * (g - delta_ref[pl.ds(bb, 1), :])).astype(BF)
        p_out[...] = p.astype(BF)

        oat = pl.multiple_of(ot * KT, KT)
        ds, pp = d_in[...], p_in[...]
        key = lax.dot_general(ds, qt_ref[ob], NT, preferred_element_type=F32)
        val = lax.dot_general(pp, do_ref[ob], NN, preferred_element_type=F32)
        acc_ref[pl.ds(oat, KT), :RANK] += key[:, :RANK] * SCALE + val
        acc_ref[pl.ds(oat, KT), RANK:] += key[:, RANK:] * SCALE
        dq = lax.dot_general(kt_ref[:, pl.ds(oat, KT)], ds, NN, preferred_element_type=F32)
        dqt_ref[ob] = dq + jnp.where(fresh, 0.0, dqt_ref[ob])
        more = (t + 1) * KT <= limit
        nextb = jnp.where(more, b, jnp.minimum(b + 1, nb))
        nextt = jnp.where(more, t + 1, 0)
        return nextb, nextt, bb, t, jnp.logical_and(t == 0, b < nb)

    def trip(_, carry):
        carry = step(*carry, p1, d1, p0, d0)
        return step(*carry, p0, d0, p1, d1)

    for b in range(nb):
        pltpu.make_async_copy(qt_hbm.at[b], qt_ref.at[b], load_s.at[b]).wait()
    steps = 1
    for b in range(nb):
        steps = steps + par_ref[b * per] // KT + 1
    lax.fori_loop(0, (steps + 1) // 2, trip, (0, 0, 0, 0, False))

    run = dq_ref.shape[2] // nb
    for b in range(nb):
        block = (dqt_ref[b] * SCALE).astype(BF)
        for h in range(nb):
            dq_ref[h, :, b * run:(b + 1) * run] = block[:, h * run:(h + 1) * run]
        if b == nb // 2 - 1 or b == nb - 1:
            half = b // (nb // 2)
            lanes = slice(half * 128, half * 128 + 128)
            pltpu.make_async_copy(dq_ref.at[:, :, lanes], dq_hbm.at[:, :, lanes], out_s.at[half]).start()
    core = lax.rem(lax.axis_index("ba"), 2)
    for g in range(8):
        mine = pl.multiple_of(g * 128 + core * 64, 64)
        other = pl.multiple_of(g * 128 + (1 - core) * 64, 64)
        part_ref[g] = acc_ref[pl.ds(other, 64), :].astype(BF)
        own_ref[g] = acc_ref[pl.ds(mine, 64), :]
    for half in range(2):
        lanes = slice(half * 128, half * 128 + 128)
        pltpu.make_async_copy(dq_ref.at[:, :, lanes], dq_hbm.at[:, :, lanes], out_s.at[half]).wait()


def core_attn(parents, qt, do, delta, lse, k):
    nb, width, rb = qt.shape
    keys = k.shape[0]
    vm, hbm = pl.BlockSpec(memory_space=pltpu.VMEM), pl.BlockSpec(memory_space=pltpu.HBM)
    return pl.pallas_call(
        attn_kernel,
        in_specs=[pl.BlockSpec(memory_space=pltpu.SMEM), hbm] + [vm] * 4,
        out_specs=[hbm, vm, vm],
        scratch_shapes=[
            pltpu.VMEM((keys, width), F32),
            pltpu.VMEM((width, keys), BF),
            pltpu.VMEM((nb, width, rb), F32),
            pltpu.VMEM((nb, rb), F32),
            pltpu.VMEM((nb, width, rb), BF),
            pltpu.VMEM((nb, width, rb), BF),
        ] + [pltpu.VMEM((KT, rb), BF)] * 4 + [pltpu.SemaphoreType.DMA((8,)), pltpu.SemaphoreType.DMA((2,))],
        out_shape=[
            jax.ShapeDtypeStruct((nb, width, rb), BF),
            jax.ShapeDtypeStruct((8, keys // 16, width), BF),
            jax.ShapeDtypeStruct((8, keys // 16, width), F32),
        ],
        compiler_params=pltpu.CompilerParams(vmem_limit_bytes=48 * 2**20),
    )(parents, qt, do, delta, lse, k)

def place():
    ba, ha = lax.axis_index("ba"), lax.axis_index("ha")
    core = lax.rem(ba, 2)
    z = lax.rem(ba // 2, 4)
    ylo = ba // 8
    x = lax.rem(ha, 4)
    yhi = ha // 4
    return core, x, yhi, ylo, z


def device(core, x, y, z):
    return {"ba": (lax.rem(y, 2) * 4 + z) * 2 + core, "ha": (y // 2) * 4 + x}


def meet(peers):
    barrier = pltpu.get_barrier_semaphore()
    for peer in peers:
        pl.semaphore_signal(barrier, inc=1, device_id=peer, device_id_type=MESH)
    pl.semaphore_wait(barrier, len(peers))


def send(src, dst, send_sem, recv_sem, peer):
    return pltpu.make_async_remote_copy(
        src_ref=src, dst_ref=dst, send_sem=send_sem, recv_sem=recv_sem,
        device_id=peer, device_id_type=MESH,
    )


def prepare(b, perm, q_in, do_in, os_in, qt_ref, do_ref, delta_ref):
    heads, _, tokens = q_in.shape
    run = tokens // heads
    lanes = slice(b * run, (b + 1) * run)
    qt_ref[b] = jnp.concatenate([q_in[h, :, lanes] for h in range(heads)], axis=1)
    rows = slice(b * tokens, (b + 1) * tokens)
    grad = lax.dot_general(perm, do_in[rows, :], NN, preferred_element_type=F32)
    saved = lax.dot_general(perm, os_in[rows, :], NN, preferred_element_type=F32)
    do_ref[b] = grad.astype(BF)
    prod = grad * saved
    part = prod[:, 0:128]
    for i in range(1, RANK // 128):
        part = part + prod[:, i * 128:(i + 1) * 128]
    delta_ref[b:b + 1, :] = jnp.sum(part.T, axis=0, keepdims=True)


def gather_kernel(lat_ref, q_hbm, do_hbm, os_hbm, out_ref, qt_ref, do_ref, delta_ref,
                  q_in, do_in, os_in, qt_s, plane_s, plane_r, line_s, line_r, pair_s, pair_r, load_s, out_s):
    loads = [
        pltpu.make_async_copy(src, dst, load_s.at[n])
        for n, (src, dst) in enumerate(((q_hbm, q_in), (do_hbm, do_in), (os_hbm, os_in)))
    ]
    for load in loads:
        load.start()
    core, x, yhi, ylo, z = place()
    y = yhi * 2 + ylo
    first = core == 0
    u, w = jnp.where(first, x, z), jnp.where(first, z, x)

    def at(du, dy, dw):
        pu, pw = lax.rem(u + du, 4), lax.rem(w + dw, 4)
        return device(core, jnp.where(first, pu, pw), lax.rem(y + dy, 4), jnp.where(first, pw, pu))

    partner = device(1 - core, x, y, z)
    plane = [(du, dy) for dy in (0, 2, 1, 3) for du in (2, 1, 3, 0) if du or dy]
    meet([at(du, dy, 0) for du, dy in plane] + [at(0, 0, dw) for dw in (1, 2, 3)] + [partner])
    mine = out_ref.at[ylo, z, core, yhi, x]
    copies = {}
    for n, (du, dy) in enumerate(plane):
        copy = send(lat_ref, mine, plane_s.at[n], plane_r.at[n], at(du, dy, 0))
        copy.start()
        copies[du, dy] = copy
    out_ref[ylo, z, core, yhi, x] = lat_ref[...]
    for load in loads:
        load.wait()
    heads, _, tokens = q_in.shape
    row = lax.broadcasted_iota(jnp.int32, (tokens, tokens), 0)
    col = lax.broadcasted_iota(jnp.int32, (tokens, tokens), 1)
    run = tokens // heads
    perm = jnp.where(col == lax.rem(row, run) * heads + row // run, 1.0, 0.0).astype(BF)

    def ready(lo, hi):
        for b in range(lo, hi):
            prepare(b, perm, q_in, do_in, os_in, qt_s, do_ref, delta_ref)
            pltpu.make_async_copy(qt_s.at[b], qt_ref.at[b], out_s.at[b]).start()

    def block(c, k, dy):
        row_y = lax.rem(y + 4 - dy, 4)
        hi, lo = row_y // 2, lax.rem(row_y, 2)
        return out_ref.at[lo, k, 0, hi] if c == 0 else out_ref.at[lo, :, 1, hi, k]

    def line_copy(c, dw, dy, k, hop):
        n = (dw - 1) * 4 + dy
        return send(block(c, k, dy), block(c, k, dy), line_s.at[n], line_r.at[n], at(0, 0, hop))

    def pair_copy(c, dw, dy):
        n, k = dw * 4 + dy, lax.rem(w + 4 - dw, 4)
        return send(block(c, k, dy), block(c, k, dy), pair_s.at[n], pair_r.at[n], partner)

    order, relayed = (0, 1, 3, 2), (0, 1)
    ready(0, 2)
    for dy in order:
        for du in (0, 1, 3, 2):
            if du or dy:
                copies[du, dy].wait_recv()
        for c in (0, 1):
            @pl.when(core == c)
            def _():
                for dw in (1, 3) if dy in relayed else (2, 1, 3):
                    line_copy(c, dw, dy, w, dw).start()
                pair_copy(c, 0, dy).start()
    ready(2, 4)
    for c in (0, 1):
        @pl.when(core == c)
        def _():
            for dy in relayed:
                line_copy(c, 3, dy, w, 3).wait_recv()
                line_copy(c, 2, dy, lax.rem(w + 1, 4), 3).start()
                pair_copy(c, 3, dy).start()
    ready(4, heads)
    for c in (0, 1):
        @pl.when(core == c)
        def _():
            for dy in order:
                for dw in (1, 3):
                    if dw == 3 and dy in relayed:
                        continue
                    line_copy(c, dw, dy, w, dw).wait_recv()
                    pair_copy(c, dw, dy).start()
            for dy in order:
                line_copy(c, 2, dy, w, 2).wait_recv()
                pair_copy(c, 2, dy).start()
            for dy in order:
                for dw in (1, 2, 3):
                    line_copy(c, dw, dy, w, dw).wait_send()
                for dw in range(4):
                    pair_copy(c, dw, dy).wait()

    for copy in copies.values():
        copy.wait_send()
    for b in range(heads):
        pltpu.make_async_copy(qt_s.at[b], qt_ref.at[b], out_s.at[b]).wait()


def gather(latents, q, do, osv):
    rows, width = latents.shape
    heads, _, tokens = q.shape
    vm, hbm = pl.BlockSpec(memory_space=pltpu.VMEM), pl.BlockSpec(memory_space=pltpu.HBM)
    return pl.pallas_call(
        gather_kernel,
        out_shape=[
            jax.ShapeDtypeStruct((2, 4, 2, 2, 4, rows, width), BF),
            jax.ShapeDtypeStruct((heads, width, tokens), BF),
            jax.ShapeDtypeStruct((heads, tokens, RANK), BF),
            jax.ShapeDtypeStruct((heads, tokens), F32),
        ],
        in_specs=[vm, hbm, hbm, hbm],
        out_specs=[vm, hbm, vm, vm],
        scratch_shapes=[pltpu.VMEM(a.shape, BF) for a in (q, do, osv, q)]
        + [pltpu.SemaphoreType.DMA((n,)) for n in (15, 15, 12, 12, 16, 16, 3, 8)],
        compiler_params=pltpu.CompilerParams(
            collective_id=0, has_side_effects=True, vmem_limit_bytes=50 * 2**20
        ),
    )(latents, q, do, osv)


def total(*blocks):
    out = blocks[0].astype(F32)
    for block in blocks[1:]:
        out = out + block.astype(F32)
    return out


def reduce_kernel(part_ref, own_ref, hid_ref, rows_ref, left_ref, hall_ref,
                  cols_ref, got0, acc0, got1, fwd, acc1, keep1, got2, acc2, colbuf, gotr, gotc,
                  s0, r0, s1, r1, s2, r2, s3, r3, s3c, r3c, s4, r4, s4c, r4c, sh, rh, sp, rp, lsem):
    core, x, yhi, ylo, z = place()
    y = yhi * 2 + ylo
    g, ha = ylo * 4 + z, yhi * 4 + x
    partner = device(1 - core, x, y, z)
    heads = [(dy, dx) for dy in (0, 1) for dx in range(4) if dy or dx]
    heads.sort(key=lambda d: -(2 * d[0] + min(d[1], 4 - d[1])))
    chips = [(dy, dz) for dy in (0, 1) for dz in range(4) if dy or dz]
    chips.sort(key=lambda d: -(d[0] + min(d[1], 4 - d[1])))

    def head_at(dy, dx):
        py, px = lax.rem(yhi + dy, 2), lax.rem(x + dx, 4)
        return py * 4 + px, device(core, px, py * 2 + ylo, z)

    def chip_at(dy, dz):
        py, pz = lax.rem(ylo + dy, 2), lax.rem(z + dz, 4)
        return py * 4 + pz, device(core, x, yhi * 2 + py, pz)

    meet([partner] + [head_at(*d)[1] for d in heads] + [chip_at(*d)[1] for d in chips])

    opp, right, left = lax.rem(x + 2, 4), lax.rem(x + 1, 4), lax.rem(x + 3, 4)
    chunks = (opp, right, left, x)

    def swap_copy(n):
        return send(part_ref.at[:, :, chunks[n]], got0.at[n], s0.at[n], r0.at[n], partner)

    for n in range(4):
        swap_copy(n).start()
    own_hidden = pltpu.make_async_copy(hid_ref, hall_ref.at[core, :, g], lsem)
    own_hidden.start()
    hidden = []
    for n, d in enumerate(chips):
        copy = send(hid_ref, hall_ref.at[core, :, g], sh.at[n], rh.at[n], chip_at(*d)[1])
        copy.start()
        hidden.append(copy)
    def paired(n, py):
        return total(own_ref[:, py, chunks[n]], got0[n, :, py])

    def line_copy(n, src, dst, dx):
        return send(src, dst, s1.at[n], r1.at[n], head_at(0, dx)[1])

    line = [
        line_copy(0, acc0.at[1, 0], got1.at[0, 0], 1),
        line_copy(1, acc0.at[1, 1], got1.at[0, 1], 1),
        line_copy(2, acc0.at[2, 0], got1.at[1, 0], 3),
        line_copy(3, acc0.at[2, 1], got1.at[1, 1], 3),
        line_copy(4, acc0.at[0, 0], fwd.at[0], 1),
        line_copy(5, acc0.at[0, 1], fwd.at[1], 3),
    ]
    swap_copy(0).wait_recv()
    acc0[0, 0] = paired(0, 0).astype(BF)
    line[4].start()
    acc0[0, 1] = paired(0, 1).astype(BF)
    line[5].start()
    swap_copy(1).wait_recv()
    acc0[1, 1] = paired(1, 1).astype(BF)
    line[1].start()
    swap_copy(2).wait_recv()
    acc0[2, 0] = paired(2, 0).astype(BF)
    line[2].start()
    swap_copy(3).wait_recv()
    for py in range(2):
        keep1[py] = paired(3, py)
    line[4].wait_recv()
    acc0[1, 0] = (paired(1, 0) + fwd[0].astype(F32)).astype(BF)
    line[0].start()
    line[5].wait_recv()
    acc0[2, 1] = (paired(2, 1) + fwd[1].astype(F32)).astype(BF)
    line[3].start()
    for n in range(4):
        line[n].wait_recv()
    acc1[...] = total(keep1[1 - yhi], got1[0, 1 - yhi], got1[1, 1 - yhi]).astype(BF)
    other = send(acc1, got2, s2, r2, head_at(1, 0)[1])
    other.start()
    keep1[yhi] = total(keep1[yhi], got1[0, yhi], got1[1, yhi])
    other.wait_recv()
    summed = total(keep1[yhi], got2[...])
    keep1[0] = summed
    acc2[...] = summed.astype(BF)
    flat = summed.reshape(64, summed.shape[-1]).T
    for k in range(8):
        pair = [flat[k * 72 + n * 36:k * 72 + n * 36 + 36, :] for n in (0, 1)]
        colbuf[k, 0:36, :] = jnp.concatenate(pair, axis=1).astype(BF)
        colbuf[k, 36:40, :] = jnp.zeros((4, 128), BF)
    rows, cols = [], []
    for n, d in enumerate(chips):
        to, peer = chip_at(*d)
        copy = send(acc2.at[to], gotr.at[n], s3.at[n], r3.at[n], peer)
        copy.start()
        rows.append(copy)
        copy = send(colbuf.at[to], gotc.at[n], s3c.at[n], r3c.at[n], peer)
        copy.start()
        cols.append(copy)
    for copy in hidden:
        copy.wait_recv()
    own_hidden.wait()
    swap = send(hall_ref.at[core], hall_ref.at[core], sp.at[0], rp.at[0], partner)
    swap.start()
    for copy in rows + cols:
        copy.wait_recv()
    rows_ref[ha] = total(keep1[0, g], *[gotr[n] for n in range(7)]).astype(BF)
    cols_ref[core, ha] = total(colbuf[g], *[gotc[n] for n in range(7)]).astype(BF)
    spread = []
    for n, d in enumerate(heads):
        _, peer = head_at(*d)
        copy = send(rows_ref.at[ha], rows_ref.at[ha], s4.at[n], r4.at[n], peer)
        copy.start()
        spread.append(copy)
        copy = send(cols_ref.at[core, ha], cols_ref.at[core, ha], s4c.at[n], r4c.at[n], peer)
        copy.start()
        spread.append(copy)
    for copy in spread:
        copy.wait_recv()
    last = send(cols_ref.at[core], cols_ref.at[core], sp.at[1], rp.at[1], partner)
    last.start()
    for n in range(4):
        swap_copy(n).wait_send()
    for copy in hidden + line + [other] + rows + cols + spread:
        copy.wait_send()
    swap.wait()
    last.wait()
    for n in range(0, 16, 2):
        both = [cols_ref[m // 8, m % 8].astype(F32) for m in (n, n + 1)]
        here = [jnp.where(core == 0, b[:, 0:64], b[:, 64:128]) for b in both]
        left_ref[:, n * 64:n * 64 + 128] = jnp.concatenate(here, axis=1).astype(BF)


def reduce_and_spread(part, own, hidden):
    width, columns = part.shape[-1], hidden.shape[-1]
    dma = pltpu.SemaphoreType.DMA
    return pl.pallas_call(
        reduce_kernel,
        out_shape=[
            jax.ShapeDtypeStruct((8, 8, width), BF),
            jax.ShapeDtypeStruct((40, 1024), BF),
            jax.ShapeDtypeStruct((2, 8, 8, 8, columns), BF),
        ],
        in_specs=[pl.BlockSpec(memory_space=pltpu.VMEM)] * 3,
        out_specs=[pl.BlockSpec(memory_space=pltpu.VMEM)] * 3,
        scratch_shapes=[
            pltpu.VMEM((2, 8, 40, 128), BF),
            pltpu.VMEM((4, 8, 2, 8, width), BF),
            pltpu.VMEM((3, 2, 8, 8, width), BF),
            pltpu.VMEM((2, 2, 8, 8, width), BF),
            pltpu.VMEM((2, 8, 8, width), BF),
            pltpu.VMEM((8, 8, width), BF),
            pltpu.VMEM((2, 8, 8, width), F32),
            pltpu.VMEM((8, 8, width), BF),
            pltpu.VMEM((8, 8, width), BF),
            pltpu.VMEM((8, 40, 128), BF),
            pltpu.VMEM((7, 8, width), BF),
            pltpu.VMEM((7, 40, 128), BF),
            dma((4,)), dma((4,)), dma((6,)), dma((6,)), dma, dma, dma((7,)), dma((7,)), dma((7,)), dma((7,)),
            dma((7,)), dma((7,)), dma((7,)), dma((7,)), dma((7,)), dma((7,)), dma((2,)), dma((2,)), dma,
        ],
        compiler_params=pltpu.CompilerParams(
            collective_id=1, has_side_effects=True, vmem_limit_bytes=20 * 2**20
        ),
    )(part, own, hidden)


def on_device(queries, out_grad, out_saved, logsumexp, parents, latents, hidden, latent_weight):
    tokens, heads, width = queries.shape
    rows = tokens * heads
    keys, qt, do, delta = gather(
        latents, queries.transpose(1, 2, 0),
        out_grad.reshape(rows, RANK), out_saved.reshape(rows, RANK),
    )
    query_grad, part, own = core_attn(
        parents, qt, do, delta, logsumexp.T, keys.reshape(-1, width)
    )
    shape = (8, 2, 4, 8, width)
    row_block, cols, hidden_all = reduce_and_spread(
        part.reshape(shape), own.reshape(shape), hidden.reshape(8, 8, -1)
    )
    weight_grad = jnp.dot(
        cols[:36], hidden_all.reshape(1024, -1), preferred_element_type=F32
    ).astype(BF)
    input_grad = jnp.dot(
        row_block.reshape(64, width), latent_weight, preferred_element_type=F32
    ).astype(BF)
    return query_grad.transpose(2, 0, 1), weight_grad, input_grad


def solution(mesh):
    return jax.shard_map(
        on_device,
        mesh=mesh,
        in_specs=(
            P("ba", "ha", None),
            P("ba", "ha", None),
            P("ba", "ha", None),
            P("ba", "ha"),
            P("ba"),
            P(("ba", "ha"), None),
            P("ba", "ha"),
            P(None, "ha"),
        ),
        out_specs=(P("ba", "ha", None), P("ba", "ha"), P("ba", "ha")),
        check_vma=False,
    )
```
